8 devices in a mesh: tp: 2 (over z, y), fsdp: 4 (over x, core).
Axes of the slice: x: 2, y: 2, z: 1, core: 2. Of those that a mesh axis runs over, the one named last changes fastest.
Arguments:
- resid_in: bfloat16 [8, 6144, 3584], P('fsdp', 'tp')
- grad_out: bfloat16 [8, 6144, 3584], P('fsdp', 'tp')
- norm_gain: float32 [3584], replicated
- w_qkv: bfloat16 [3584, 4608], P('fsdp', 'tp')
- b_qkv: bfloat16 [4608], P('tp')
- sinks: float32 [28], P('tp')
- w_out: bfloat16 [3584, 3584], P(('tp', 'fsdp'))
- b_out: bfloat16 [3584], replicated
Outputs:
- output 1: bfloat16 [8, 6144, 3584], P('fsdp', 'tp')
- output 2: bfloat16 [8, 6144, 3584], P('fsdp', 'tp')
- output 3: float32 [3584], replicated
- output 4: float32 [3584, 4608], P('fsdp', 'tp')
- output 5: float32 [4608], P('tp')
- output 6: float32 [28], P('tp')
- output 7: float32 [3584, 3584], P(('tp', 'fsdp'))
- output 8: float32 [3584], replicated
All inputs are finite; a program needn't handle non-finite values.
Results may differ from the reference program's by a relative error of at most 0.0114246.
Values are sent between devices in bfloat16 or wider.
A program may use at most 1 GiB of HBM per device.

```python
import jax
import jax.numpy as jnp
from jax import lax

D = 3584
HEADS = 28
KV_HEADS = 4
HEAD = 128
WINDOW = 128
BATCH = 8
SEQ = 6144

GROUP = HEADS // KV_HEADS
QKV_COLS = (HEADS + 2 * KV_HEADS) * HEAD
N_BLOCKS = SEQ // WINDOW
EPS = 1e-5
ROPE_BASE = 150000.0


def setup_inputs(seed: int = 0) -> dict:
    rng_keys = jax.random.split(jax.random.key(seed), 8)
    resid_in = jax.random.normal(rng_keys[0], (BATCH, SEQ, D), jnp.float32)
    grad_out = jax.random.normal(rng_keys[1], (BATCH, SEQ, D), jnp.float32)
    norm_gain = 1.0 + 0.3 * jax.random.normal(rng_keys[2], (D,), jnp.float32)
    w_qkv = (1.2 / D ** 0.5) * jax.random.normal(rng_keys[3], (D, QKV_COLS), jnp.float32)
    b_qkv = 0.5 * jax.random.normal(rng_keys[4], (QKV_COLS,), jnp.float32)
    sinks = 5.0 + 1.5 * jax.random.normal(rng_keys[5], (HEADS,), jnp.float32)
    w_out = (1.5 / (HEADS * HEAD) ** 0.5) * jax.random.normal(rng_keys[6], (HEADS * HEAD, D), jnp.float32)
    b_out = 0.5 * jax.random.normal(rng_keys[7], (D,), jnp.float32)
    return {
        "resid_in": resid_in.astype(jnp.bfloat16),
        "grad_out": grad_out.astype(jnp.bfloat16),
        "norm_gain": norm_gain,
        "w_qkv": w_qkv.astype(jnp.bfloat16),
        "b_qkv": b_qkv.astype(jnp.bfloat16),
        "sinks": sinks,
        "w_out": w_out.astype(jnp.bfloat16),
        "b_out": b_out.astype(jnp.bfloat16),
    }


def rope_tables(length):
    positions = jnp.arange(length).astype(jnp.float32)
    inv_freq = ROPE_BASE ** (-2.0 * jnp.arange(HEAD // 2).astype(jnp.float32) / HEAD)
    angles = positions[:, None] * inv_freq[None, :]
    return jnp.cos(angles), jnp.sin(angles)


def apply_rope(head_vals, cos_tab, sin_tab):
    half_dim = head_vals.shape[-1] // 2
    first_half = head_vals[..., :half_dim]
    second_half = head_vals[..., half_dim:]
    return jnp.concatenate([first_half * cos_tab - second_half * sin_tab, second_half * cos_tab + first_half * sin_tab], axis=-1)


def block_attend(block_in, sinks):
    q_blk, k_blk, v_blk, block_idx = block_in
    scores = jnp.einsum("iegd,jed->egij", q_blk, k_blk) / HEAD ** 0.5
    q_idx = jnp.arange(WINDOW)[:, None]
    k_idx = jnp.arange(2 * WINDOW)[None, :]
    allowed = (k_idx > q_idx) & (k_idx <= q_idx + WINDOW) & (block_idx * WINDOW - WINDOW + k_idx >= 0)
    scores = jnp.where(allowed, scores, -1e30)
    sink_col = sinks.reshape(KV_HEADS, GROUP)[:, :, None, None]
    row_max = lax.stop_gradient(jnp.maximum(jnp.max(scores, axis=-1, keepdims=True), sink_col))
    exp_scores = jnp.exp(scores - row_max)
    row_denom = jnp.sum(exp_scores, axis=-1, keepdims=True) + jnp.exp(sink_col - row_max)
    attn_probs = (exp_scores / row_denom).astype(jnp.bfloat16).astype(jnp.float32)
    return jnp.einsum("egij,jed->iegd", attn_probs, v_blk)


def row_forward(resid_row, params):
    norm_gain, w_qkv, b_qkv, sinks, w_out, b_out = params
    mean_sq = jnp.mean(resid_row * resid_row, axis=-1, keepdims=True)
    normed = (resid_row * lax.rsqrt(mean_sq + EPS) * norm_gain).astype(jnp.bfloat16).astype(jnp.float32)
    qkv_proj = (jnp.dot(normed, w_qkv, preferred_element_type=jnp.float32) + b_qkv).astype(jnp.bfloat16).astype(jnp.float32)
    qkv_proj = qkv_proj.reshape(SEQ, KV_HEADS, GROUP + 2, HEAD)
    cos_tab, sin_tab = rope_tables(SEQ)
    queries = apply_rope(qkv_proj[:, :, :GROUP], cos_tab[:, None, None], sin_tab[:, None, None]).astype(jnp.bfloat16).astype(jnp.float32)
    keys_rot = apply_rope(qkv_proj[:, :, GROUP], cos_tab[:, None], sin_tab[:, None]).astype(jnp.bfloat16).astype(jnp.float32)
    values = qkv_proj[:, :, GROUP + 1]
    zero_pad = jnp.zeros((WINDOW, KV_HEADS, HEAD), jnp.float32)
    k_prev = jnp.concatenate([zero_pad, keys_rot[:SEQ - WINDOW]], axis=0).reshape(N_BLOCKS, WINDOW, KV_HEADS, HEAD)
    v_prev = jnp.concatenate([zero_pad, values[:SEQ - WINDOW]], axis=0).reshape(N_BLOCKS, WINDOW, KV_HEADS, HEAD)
    k_blocks = jnp.concatenate([k_prev, keys_rot.reshape(N_BLOCKS, WINDOW, KV_HEADS, HEAD)], axis=1)
    v_blocks = jnp.concatenate([v_prev, values.reshape(N_BLOCKS, WINDOW, KV_HEADS, HEAD)], axis=1)
    q_blocks = queries.reshape(N_BLOCKS, WINDOW, KV_HEADS, GROUP, HEAD)
    attend = jax.checkpoint(block_attend)
    attn_out = lax.map(lambda block_in: attend(block_in, sinks), (q_blocks, k_blocks, v_blocks, jnp.arange(N_BLOCKS)))
    attn_out = attn_out.reshape(SEQ, HEADS * HEAD).astype(jnp.bfloat16).astype(jnp.float32)
    resid_out = resid_row + jnp.dot(attn_out, w_out, preferred_element_type=jnp.float32) + b_out
    return resid_out.astype(jnp.bfloat16)


def reference(resid_in, grad_out, norm_gain, w_qkv, b_qkv, sinks, w_out, b_out):
    params = (norm_gain, w_qkv.astype(jnp.float32), b_qkv.astype(jnp.float32), sinks, w_out.astype(jnp.float32), b_out.astype(jnp.float32))

    def row_step(grad_acc, row_in):
        resid_row, grad_row = row_in
        resid_out, pullback = jax.vjp(row_forward, resid_row.astype(jnp.float32), params)
        d_resid, row_grads = pullback(grad_row)
        new_acc = tuple(acc_sum + new_grad for acc_sum, new_grad in zip(grad_acc, row_grads))
        return new_acc, (resid_out, d_resid.astype(jnp.bfloat16))

    zero_acc = tuple(jnp.zeros_like(param_val) for param_val in params)
    grad_sums, (resid_rows, grad_rows) = lax.scan(row_step, zero_acc, (resid_in, grad_out))
    return (resid_rows, grad_rows, grad_sums[0], grad_sums[1], grad_sums[2], grad_sums[3], grad_sums[4], grad_sums[5])
```

```python
import functools

import jax
import jax.numpy as jnp
from jax import lax
from jax.experimental import pallas as pl
from jax.experimental.pallas import tpu as pltpu
from jax.sharding import PartitionSpec as P

EPS = 1e-5
ROPE_BASE = 150000.0
W = 128
HD = 128
GROUP = 7
COLS = (GROUP + 2) * HD
QCOLS = GROUP * HD
SCALE = HD ** -0.5
LOG2E = 1.4426950408889634
NEG = -1e30
F32 = jnp.float32
BF16 = jnp.bfloat16
NT = (((1,), (1,)), ((), ()))
NN = (((1,), (0,)), ((), ()))
HEAD_SETS = ((0, 1), (2, 3), (4, 5, 6))
VMEM_LIMIT = 66_000_000


def rope_tables(positions, head_dim):
    inv_freq = ROPE_BASE ** (-2.0 * jnp.arange(head_dim // 2).astype(F32) / head_dim)
    angles = positions.astype(F32)[:, None] * inv_freq[None, :]
    return jnp.cos(angles), jnp.sin(angles)


def rope_back(head_grads, cos_tab, sin_tab):
    half_dim = head_grads.shape[-1] // 2
    first_half = head_grads[..., :half_dim]
    second_half = head_grads[..., half_dim:]
    return jnp.concatenate([first_half * cos_tab + second_half * sin_tab, second_half * cos_tab - first_half * sin_tab], axis=-1)


def dot(a, b, dims):
    return lax.dot_general(a, b, dims, preferred_element_type=F32)


def attn_body(n_blocks, flags, sinks, qkv, d_attn, halo, cos2, sin2, cos_t, sin_t, upper_bf, _, attn, d_qkv, dkv_halo, dkv_last, col_sum, d_sink, k_cat, v_cat, k_t, v_t, dk_acc, dv_acc):
    group = pl.program_id(1)
    has_prev = flags[0] > 0
    row = lax.broadcasted_iota(jnp.int32, (W, W), 0)
    col = lax.broadcasted_iota(jnp.int32, (W, W), 1)
    upper = row > col

    k_halo = halo[0, 0, :, :HD].astype(F32)
    k_halo = (k_halo * cos2[:W, :] + pltpu.roll(k_halo, HD // 2, 1) * sin2[:W, :]).astype(BF16)
    k_cat[W:, :] = k_halo
    v_cat[W:, :] = halo[0, 0, :, HD:]
    k_t[:, W:] = k_halo.T
    v_t[:, W:] = halo[0, 0, :, HD:].T
    dk_acc[...] = jnp.zeros_like(dk_acc)
    dv_acc[...] = jnp.zeros_like(dv_acc)
    col_sum[...] = jnp.zeros_like(col_sum)
    d_sink[...] = jnp.zeros_like(d_sink)

    def block(b, first):
        r0 = 0 if first else pl.multiple_of(b * W, W)
        rows = pl.ds(r0, W)
        tab_rows = pl.ds(r0 + W, W)
        cos_b, sin_b = cos2[tab_rows, :], sin2[tab_rows, :]
        cos_c, sin_c = cos_t[:, rows], sin_t[:, rows]

        def rotate(raw):
            wide = raw.astype(F32)
            return (wide * cos_b + pltpu.roll(wide, HD // 2, 1) * sin_b).astype(BF16)

        k_new = rotate(qkv[rows, QCOLS:QCOLS + HD])
        v_new = qkv[rows, QCOLS + HD:]
        k_cat[:W, :] = k_cat[W:, :]
        v_cat[:W, :] = v_cat[W:, :]
        k_t[:, :W] = k_t[:, W:]
        v_t[:, :W] = v_t[:, W:]
        k_cat[W:, :] = k_new
        v_cat[W:, :] = v_new
        k_t[:, W:] = k_new.T
        v_t[:, W:] = v_new.T
        keys, values = k_cat[...], v_cat[...]
        keys_t, values_t = k_t[...], v_t[...]
        mask_bf = upper_bf[...]

        dk, dv = [], []

        def ahead(heads):
            q_set = jnp.concatenate([rotate(qkv[rows, h * HD:(h + 1) * HD]) for h in heads], axis=0)
            do_set = jnp.concatenate([d_attn[rows, h * HD:(h + 1) * HD] for h in heads], axis=0)
            return q_set, do_set, dot(keys, q_set, NT), dot(values, do_set, NT)

        def softmax(heads, q_set, do_set, scores, d_prob2):
            probs, d_scores = [], []
            for i, h in enumerate(heads):
                lanes = slice(i * W, (i + 1) * W)
                s_prev = scores[:W, lanes]
                if first:
                    s_prev = jnp.where(has_prev, s_prev, NEG)
                s = jnp.where(upper, s_prev, scores[W:, lanes])
                s = s * (SCALE * LOG2E)
                sink = sinks[group * GROUP + h] * LOG2E
                top = jnp.maximum(jnp.max(s, axis=0, keepdims=True), sink)
                e = jnp.exp2(s - top)
                e_sink = jnp.exp2(sink - top)
                inv = 1.0 / (jnp.sum(e, axis=0, keepdims=True) + e_sink)
                p = e * inv
                dp = jnp.where(upper, d_prob2[:W, lanes], d_prob2[W:, lanes]).astype(BF16).astype(F32)
                row_dot = jnp.sum(p * dp, axis=0, keepdims=True)
                d_sink[0, 0, h:h + 1, :] -= (e_sink * inv) * row_dot
                p_bf = p.astype(BF16)
                ds_bf = (p * (dp - row_dot)).astype(BF16)
                p_prev = p_bf * mask_bf
                ds_prev = ds_bf * mask_bf
                probs.append(jnp.concatenate([p_prev, p_bf - p_prev], axis=0))
                d_scores.append(jnp.concatenate([ds_prev, ds_bf - ds_prev], axis=0))
            return q_set, do_set, jnp.concatenate(probs, axis=1), jnp.concatenate(d_scores, axis=1)

        def behind(heads, q_set, do_set, p_set, ds_set):
            dv.append(dot(p_set, do_set, NN))
            dk.append(dot(ds_set, q_set, NN))
            return dot(values_t, p_set, NN), dot(keys_t, ds_set, NN)

        def store(heads, out_t, dq_t):
            for i, h in enumerate(heads):
                lanes = slice(i * W, (i + 1) * W)
                cols = slice(h * HD, (h + 1) * HD)
                attn[rows, cols] = out_t[:, lanes].astype(BF16).T
                g = (dq_t[:, lanes] * SCALE).astype(BF16).astype(F32)
                g1, g2 = g[:HD // 2], g[HD // 2:]
                dq = jnp.concatenate([g1 * cos_c + g2 * sin_c, g2 * cos_c - g1 * sin_c], axis=0).astype(BF16).T
                d_qkv[rows, cols] = dq
                col_sum[0, 0, 0:1, cols] += jnp.sum(dq.astype(F32), axis=0, keepdims=True)

        stages = (ahead, softmax, behind, store)
        held = [()] * len(HEAD_SETS)
        for tick in range(len(HEAD_SETS) + len(stages) - 1):
            for k in range(len(stages)):
                i = tick - k
                if 0 <= i < len(HEAD_SETS):
                    held[i] = stages[k](HEAD_SETS[i], *held[i])
        dk, dv = sum(dk[1:], dk[0]), sum(dv[1:], dv[0])

        if first:
            dkv_halo[0, 0, :, :HD] = dk[:W]
            dkv_halo[0, 0, :, HD:] = dv[:W]
        else:
            done = pl.ds(pl.multiple_of(b * W - W, W), W)
            g = ((dk_acc[...] + dk[:W]) * SCALE).astype(BF16).astype(F32)
            dk_out = (g * cos2[rows, :] - pltpu.roll(g, HD // 2, 1) * sin2[rows, :]).astype(BF16)
            dv_out = (dv_acc[...] + dv[:W]).astype(BF16)
            d_qkv[done, QCOLS:QCOLS + HD] = dk_out
            d_qkv[done, QCOLS + HD:] = dv_out
            col_sum[0, 0, 0:1, QCOLS:QCOLS + HD] += jnp.sum(dk_out.astype(F32), axis=0, keepdims=True)
            col_sum[0, 0, 0:1, QCOLS + HD:] += jnp.sum(dv_out.astype(F32), axis=0, keepdims=True)
        dk_acc[...] = dk[W:]
        dv_acc[...] = dv[W:]

    block(0, True)

    def step(b, carry):
        block(b, False)
        return carry

    lax.fori_loop(1, n_blocks, step, 0)
    dkv_last[0, 0, :, :HD] = dk_acc[...]
    dkv_last[0, 0, :, HD:] = dv_acc[...]
    last = pl.ds((n_blocks - 1) * W, W)
    d_qkv[last, QCOLS:] = jnp.zeros((W, 2 * HD), BF16)


def attention(piece, flags, sinks, qkv, d_attn, halo, cos2, sin2, attn_buf, n_rows, seq):
    tokens = n_rows * seq
    groups = qkv.shape[1] // COLS
    upper_bf = (jnp.arange(W)[:, None] > jnp.arange(W)[None, :]).astype(BF16)
    cos_t, sin_t = cos2[W:, :HD // 2].T, sin2[W:, HD // 2:].T
    once = pl.Buffered(1)
    const = lambda *shape: pl.BlockSpec(shape, lambda n, e: (0,) * len(shape), pipeline_mode=once)
    part = lambda *shape: pl.BlockSpec((1, 1) + shape, lambda n, e: (n, e) + (0,) * len(shape))
    wide = pl.BlockSpec((seq, COLS), lambda n, e: (n, e))
    heads = pl.BlockSpec((seq, QCOLS), lambda n, e: (n, piece * groups + e))
    out_shape = (
        jax.ShapeDtypeStruct((tokens, d_attn.shape[1]), BF16),
        jax.ShapeDtypeStruct((tokens, qkv.shape[1]), BF16),
        jax.ShapeDtypeStruct((n_rows, groups, W, 2 * HD), F32),
        jax.ShapeDtypeStruct((n_rows, groups, W, 2 * HD), F32),
        jax.ShapeDtypeStruct((n_rows, groups, 8, COLS), F32),
        jax.ShapeDtypeStruct((n_rows, groups, 8, W), F32),
    )
    any_spec = pl.BlockSpec(memory_space=pl.ANY)
    smem = pl.BlockSpec(memory_space=pltpu.SMEM)
    in_specs = [smem, smem, wide, heads, part(W, 2 * HD), const(seq + W, HD), const(seq + W, HD), const(HD // 2, seq), const(HD // 2, seq), const(W, W), any_spec]
    operands = [flags, sinks, qkv, d_attn, halo, cos2, sin2, cos_t, sin_t, upper_bf, attn_buf]
    aliases = {10: 0}
    if attn_buf is None:
        operands[10] = jnp.zeros((8, 128), BF16)
        aliases = {}
    pair_macs = tokens * groups * GROUP * 2 * W * HD
    return pl.pallas_call(
        functools.partial(attn_body, seq // W),
        name=f"attention_{piece}",
        grid=(n_rows, groups),
        in_specs=in_specs,
        out_specs=(heads, wide, part(W, 2 * HD), part(W, 2 * HD), part(8, COLS), part(8, W)),
        out_shape=out_shape,
        scratch_shapes=[pltpu.VMEM((2 * W, HD), BF16)] * 2 + [pltpu.VMEM((HD, 2 * W), BF16)] * 2 + [pltpu.VMEM((W, HD), F32)] * 2,
        input_output_aliases=aliases,
        compiler_params=pltpu.CompilerParams(vmem_limit_bytes=VMEM_LIMIT),
        cost_estimate=pl.CostEstimate(flops=24 * pair_macs, bytes_accessed=8 * tokens * groups * COLS, transcendentals=tokens * groups * GROUP * W),
    )(*operands)


def norm_forward_body(x, gain, out):
    wide = x[...].astype(F32)
    inv = lax.rsqrt(jnp.mean(wide * wide, axis=-1, keepdims=True) + EPS)
    out[...] = (wide * inv * gain[0:1, :]).astype(BF16)


def norm_forward(x, gain):
    tokens, width = x.shape
    tile = min(512, tokens)
    block = pl.BlockSpec((tile, width), lambda i: (i, 0))
    return pl.pallas_call(
        norm_forward_body,
        name="norm_forward",
        grid=(tokens // tile,),
        in_specs=[block, pl.BlockSpec((8, width), lambda i: (0, 0))],
        out_specs=block,
        out_shape=jax.ShapeDtypeStruct(x.shape, BF16),
        compiler_params=pltpu.CompilerParams(vmem_limit_bytes=VMEM_LIMIT),
        cost_estimate=pl.CostEstimate(flops=4 * tokens * width, bytes_accessed=4 * tokens * width, transcendentals=tokens),
    )(x, jnp.broadcast_to(gain[None, :], (8, width)))


def norm_backward_body(dh, x, dy, gain, dx, sums):
    @pl.when(pl.program_id(0) == 0)
    def _():
        sums[...] = jnp.zeros_like(sums)

    wide = x[...].astype(F32)
    grad = dh[...].astype(F32)
    up = dy[...].astype(F32)
    inv = lax.rsqrt(jnp.mean(wide * wide, axis=-1, keepdims=True) + EPS)
    gain_grad = grad * gain[0:1, :]
    proj = jnp.mean(gain_grad * wide, axis=-1, keepdims=True)
    dx[...] = (up + inv * (gain_grad - wide * (inv * inv * proj))).astype(BF16)
    sums[0:1, :] += jnp.sum(grad * wide * inv, axis=0, keepdims=True)
    sums[1:2, :] += jnp.sum(up, axis=0, keepdims=True)


def norm_backward(dh, x, dy, gain):
    tokens, width = x.shape
    tile = min(256, tokens)
    block = pl.BlockSpec((tile, width), lambda i: (i, 0))
    small = pl.BlockSpec((8, width), lambda i: (0, 0))
    return pl.pallas_call(
        norm_backward_body,
        name="norm_backward",
        grid=(tokens // tile,),
        in_specs=[block, block, block, small],
        out_specs=(block, small),
        out_shape=(jax.ShapeDtypeStruct(x.shape, BF16), jax.ShapeDtypeStruct((8, width), F32)),
        compiler_params=pltpu.CompilerParams(vmem_limit_bytes=VMEM_LIMIT),
        cost_estimate=pl.CostEstimate(flops=12 * tokens * width, bytes_accessed=8 * tokens * width, transcendentals=tokens),
    )(dh, x, dy, jnp.broadcast_to(gain[None, :], (8, width)))


def unwritten(shape, dtype):
    return pl.pallas_call(
        lambda out: None,
        name="unwritten",
        out_specs=pl.BlockSpec(memory_space=pl.ANY),
        out_shape=jax.ShapeDtypeStruct(shape, dtype),
    )()


def solution(mesh):
    act_spec = P("fsdp", "tp", None)
    wout_spec = P(("tp", "fsdp"), None)
    in_specs = (act_spec, act_spec, P(), P("fsdp", "tp"), P("tp"), P("tp"), wout_spec, P())
    out_specs = (act_spec, act_spec, P(), P("fsdp", "tp"), P("tp"), P("tp"), wout_spec, P())
    both = ("tp", "fsdp")
    n_tp = mesh.shape["tp"]

    def device_step(resid_loc, grad_loc, norm_gain, wqkv_loc, bqkv_loc, sink_loc, wout_loc, b_out):
        n_rows, seq, width = resid_loc.shape
        tokens = n_rows * seq
        here = lax.axis_index("tp")
        x = resid_loc.reshape(tokens, width)
        dy = grad_loc.reshape(tokens, width)
        groups = wqkv_loc.shape[1] // COLS
        heads_loc = sink_loc.shape[0]

        wout = lax.all_gather(wout_loc, both, axis=0, tiled=True)
        normed = norm_forward(x, norm_gain)
        wqkv_loc, normed = lax.optimization_barrier((wqkv_loc, normed))
        wqkv = lax.all_gather(wqkv_loc, both, axis=0, tiled=True).reshape(n_tp, width, -1)
        bqkv = lax.all_gather(bqkv_loc, "tp", axis=0, tiled=True).reshape(n_tp, -1).astype(F32)
        sinks = lax.all_gather(sink_loc, "tp", axis=0, tiled=True)

        d_attn = dot(dy, wout, NT).astype(BF16)
        normed, d_attn = lax.optimization_barrier((normed, d_attn))
        cos_tab, sin_tab = rope_tables(here * seq - W + jnp.arange(seq + W), HD)
        cos2 = jnp.concatenate([cos_tab, cos_tab], axis=1)
        sin2 = jnp.concatenate([-sin_tab, sin_tab], axis=1)
        flags = here.astype(jnp.int32).reshape(1)

        qkv = [(dot(normed, wqkv[t], NN) + bqkv[t]).astype(BF16) for t in range(n_tp)]
        halos = []
        for t in range(n_tp):
            tails = [[qkv[t][(n + 1) * seq - W:(n + 1) * seq, e * COLS + QCOLS:(e + 1) * COLS] for e in range(groups)] for n in range(n_rows)]
            halos.append(lax.ppermute(jnp.stack([jnp.stack(row) for row in tails]), "tp", [(i, i + 1) for i in range(n_tp - 1)]))

        attn, d_qkv, col_sums, d_sinks = None, [], [], []
        for t in range(n_tp):
            attn, dq, dkv_halo, dkv_last, col_sum, d_sink = attention(t, flags, sinks[t * heads_loc:(t + 1) * heads_loc], qkv[t], d_attn, halos[t], cos2, sin2, attn, n_rows, seq)
            dkv = dkv_last + lax.ppermute(dkv_halo, "tp", [(i + 1, i) for i in range(n_tp - 1)])
            dk = (dkv[..., :HD] * SCALE).astype(BF16).astype(F32)
            dk = rope_back(dk, cos_tab[seq:], sin_tab[seq:]).astype(BF16)
            dkv = jnp.concatenate([dk, dkv[..., HD:].astype(BF16)], axis=-1)
            for n in range(n_rows):
                for e in range(groups):
                    dq = lax.dynamic_update_slice(dq, dkv[n, e], (n * seq + seq - W, e * COLS + QCOLS))
            d_qkv.append(dq)
            total = jnp.sum(col_sum[:, :, 0], axis=0)
            col_sums.append(total.at[:, QCOLS:].add(jnp.sum(dkv, axis=(0, 2), dtype=F32)).reshape(-1))
            d_sinks.append(jnp.sum(d_sink[:, :, :GROUP], axis=(0, 3)).reshape(-1))

        over_tokens = (((0,), (0,)), ((), ()))
        grad_wout = lax.psum_scatter(dot(attn, dy, over_tokens), both, scatter_dimension=0, tiled=True)
        wqkv_part = unwritten((n_tp * width, wqkv.shape[2]), F32)
        for t in range(n_tp):
            wqkv_part = lax.dynamic_update_slice(wqkv_part, dot(normed, d_qkv[t], over_tokens), (t * width, 0))
        grad_wqkv = lax.psum_scatter(wqkv_part, both, scatter_dimension=0, tiled=True)

        d_normed = dot(d_qkv[0], wqkv[0], NT)
        for t in range(1, n_tp):
            d_normed = d_normed + dot(d_qkv[t], wqkv[t], NT)
        grad_resid, sums = norm_backward(d_normed.astype(BF16), x, dy, norm_gain)

        resid_out = (x.astype(F32) + dot(attn, wout, NN) + b_out.astype(F32)).astype(BF16)

        small = lax.psum(jnp.concatenate([sums[0], sums[1]] + col_sums + d_sinks), both)
        n_cols = groups * COLS
        grad_gain, grad_bout = small[:width], small[width:2 * width]
        grad_bqkv = lax.dynamic_slice(small, (2 * width + here * n_cols,), (n_cols,))
        grad_sinks = lax.dynamic_slice(small, (2 * width + n_tp * n_cols + here * heads_loc,), (heads_loc,))
        return (resid_out.reshape(resid_loc.shape), grad_resid.reshape(resid_loc.shape), grad_gain, grad_wqkv, grad_bqkv, grad_sinks, grad_wout, grad_bout)

    return jax.shard_map(device_step, mesh=mesh, in_specs=in_specs, out_specs=out_specs, check_vma=False)
```
